32 devices in a mesh: pts: 8 (over z, x), help: 4 (over y, core).
Axes of the slice: x: 2, y: 2, z: 4, core: 2. Of those that a mesh axis runs over, the one named last changes fastest.
Arguments:
- src_points: bfloat16 [8192, 256], P(('pts', 'help')), may hold values from -8 to 8
- dst_points: bfloat16 [8192, 256], P(('pts', 'help')), may hold values from -8 to 8
- src_logw: float32 [8192], P(('pts', 'help')), may hold values from -1.2 to 1.2
- dst_logw: float32 [8192], P(('pts', 'help')), may hold values from -1.2 to 1.2
- init_g: float32 [8192], P(('pts', 'help')), may hold values from -2 to 7000
- pair_lists: int32 [32, 24], P(('pts', 'help')), may hold values from 0 to 31, as said below
- pair_counts: int32 [32], P(('pts', 'help')), may hold values from 3 to 24, as said below
Outputs:
- dual_f: float32 [8192], P(('pts', 'help'))
- dual_g: float32 [8192], P(('pts', 'help'))
The draws below stay inside these ranges and needn't reach their ends.
Inputs may be any that keep to these rules, and one draw needn't show every extreme that they name: `pair_lists`: row block r's first pair_counts[r] entries are distinct, one of them is r itself, and each names a block whose points are held by an index of pts at most 3 away from the index that holds r; the later entries equal r. `pair_counts`: 24 is reached by some row block in every draw. The counts of the blocks held by one index of pts sum to at most 14 times the number of help devices; dealt out in turn to the help devices of that index, they give some device exactly 24 in every draw.
All inputs are finite; a program needn't handle non-finite values.
Results may differ from the reference program's by a relative error of at most 0.0003.
Values may be sent and summed in bfloat16 or wider, within the bound.
No kernel may reach another device: no remote copies, remote signals or barrier semaphores. Data moves between devices by JAX's collectives and lax.ppermute only.
A program may use at most 64 MiB of HBM per device.

```python
import jax
import jax.numpy as jnp
from jax import lax

D = 256
BLOCK = 256
PAIR_MOST = 24
REACH = 3
ITERS = 2
BLOCKS = 32
POINTS = 8192
N_HELP = 4


def point_cloud(key):
    keys = jax.random.split(jax.random.fold_in(key, 13), 3)
    sources = 0.18 * jnp.clip(jax.random.normal(keys[0], (POINTS, D)), -4.0, 4.0)
    targets = 0.18 * jnp.clip(jax.random.normal(keys[1], (POINTS, D)), -4.0, 4.0)
    jitter = 0.25 * jnp.clip(jax.random.normal(keys[2], (POINTS,)), -3.0, 3.0)
    source_half = sources.astype(jnp.bfloat16)
    target_half = targets.astype(jnp.bfloat16)
    target_wide = target_half.astype(jnp.float32)
    potential = 0.5 * jnp.sum(target_wide * target_wide, axis=1) + jitter
    return (source_half, target_half, potential)


def draw_src_points(key, part):
    return point_cloud(key)[0]


def draw_dst_points(key, part):
    return point_cloud(key)[1]


def draw_init_g(key, part):
    return point_cloud(key)[2]


def pair_tables(key):
    keys = jax.random.split(jax.random.fold_in(key, 29), 7)
    blocks = BLOCKS
    groups = BLOCKS // N_HELP
    owners = jnp.arange(blocks) // N_HELP
    within = jnp.arange(blocks) % N_HELP
    counts = jax.random.randint(keys[0], (blocks,), 3, 11)
    heavy_on = jax.random.randint(keys[1], (groups,), 0, 4) == 0
    heavy_at = jax.random.randint(keys[2], (groups,), 0, N_HELP)
    heavy_count = jax.random.randint(keys[3], (groups,), 16, PAIR_MOST + 1)
    is_heavy = heavy_on[owners] & (heavy_at[owners] == within)
    counts = jnp.where(is_heavy, heavy_count[owners], counts)
    forced = jax.random.randint(keys[4], (), REACH, max(REACH + 1, groups - REACH))
    forced_at = jax.random.randint(keys[5], (), 0, N_HELP)
    counts = jnp.where(owners == forced, jnp.where(within == forced_at, PAIR_MOST, 10), counts)
    lowest = jnp.maximum(owners - REACH, 0)
    highest = jnp.minimum(owners + REACH, groups - 1)
    counts = jnp.minimum(counts, (highest - lowest + 1) * N_HELP)
    spot_count = (2 * REACH + 1) * N_HELP
    slots = jnp.arange(spot_count)
    col_owner = owners[:, None] - REACH + slots[None, :] // N_HELP
    columns = col_owner * N_HELP + slots[None, :] % N_HELP
    usable = (col_owner >= 0) & (col_owner < groups)
    ranking = jax.random.randint(keys[6], (blocks, spot_count), 0, 2 ** 20) * 64 + slots[None, :]
    ranking = jnp.where(usable, ranking, ranking + 2 ** 27)
    ranking = jnp.where(columns == jnp.arange(blocks)[:, None], -1, ranking)
    picked = jnp.argsort(ranking, axis=1, stable=True)[:, :PAIR_MOST]
    chosen = jnp.take_along_axis(columns, picked, axis=1)
    keeping = jnp.arange(PAIR_MOST)[None, :] < counts[:, None]
    chosen = jnp.where(keeping, chosen, jnp.arange(blocks)[:, None])
    return (chosen.astype(jnp.int32), counts.astype(jnp.int32))


def draw_pair_lists(key, part):
    return pair_tables(key)[0]


def draw_pair_counts(key, part):
    return pair_tables(key)[1]


def block_levels(stream_key, extent, cuts, smallest, largest):
    level, own = 1.0, jax.random.fold_in(stream_key, 6)
    for axis_at, shards_of in cuts:
        heights = jnp.exp(jax.random.uniform(jax.random.fold_in(own, axis_at), (shards_of,), jnp.float32, smallest / len(cuts), largest / len(cuts)))
        level = level * jnp.repeat(heights, extent[axis_at] // shards_of).reshape([-1 if axis == axis_at else 1 for axis in range(len(extent))])
    return level


def setup_inputs(seed: int = 0) -> dict:
    key_of = jax.random.split(jax.random.key(seed), 8)
    src_points = draw_src_points(jax.random.fold_in(key_of[7], 71), 0)
    dst_points = draw_dst_points(jax.random.fold_in(key_of[7], 71), 0)
    src_logw = jnp.clip(jax.random.uniform(key_of[2], (POINTS,), jnp.float32, -1.2, 1.2) * block_levels(key_of[2], (POINTS,), ((0, 32),), -0.4, 0.0), -1.2, 1.2)
    dst_logw = jnp.clip(jax.random.uniform(key_of[3], (POINTS,), jnp.float32, -1.2, 1.2) * block_levels(key_of[3], (POINTS,), ((0, 32),), -0.4, 0.0), -1.2, 1.2)
    init_g = draw_init_g(jax.random.fold_in(key_of[7], 71), 0)
    pair_lists = draw_pair_lists(jax.random.fold_in(key_of[7], 71), 0)
    pair_counts = draw_pair_counts(jax.random.fold_in(key_of[7], 71), 0)
    return {"src_points": src_points, "dst_points": dst_points, "src_logw": src_logw, "dst_logw": dst_logw, "init_g": init_g, "pair_lists": pair_lists, "pair_counts": pair_counts}


EPS = 0.25
NEGATIVE = -1.0e30


def reference(src_points, dst_points, src_logw, dst_logw, init_g, pair_lists, pair_counts):
    blocks = pair_lists.shape[0]
    src_full = src_points.astype(jnp.float32).reshape(blocks, BLOCK, D)
    dst_full = dst_points.astype(jnp.float32).reshape(blocks, BLOCK, D)
    src_half = 0.5 * jnp.sum(src_full * src_full, axis=2)
    dst_half = 0.5 * jnp.sum(dst_full * dst_full, axis=2)
    src_weight = src_logw.reshape(blocks, BLOCK)
    dst_weight = dst_logw.reshape(blocks, BLOCK)
    active = jnp.arange(PAIR_MOST, dtype=jnp.int32)[None, :] < pair_counts[:, None]
    dual_g = init_g.reshape(blocks, BLOCK)
    dual_f = jnp.zeros_like(dual_g)
    for sweep_index in range(ITERS):
        def one_block(carry, item):
            col_top, col_sum = carry
            row_pts, row_half, row_weight, columns, active_row = item
            inner_dot = jnp.einsum("nd,kmd->knm", row_pts, dst_full[columns], precision=lax.Precision.HIGHEST)
            cost_tile = row_half[None, :, None] + dst_half[columns][:, None, :] - inner_dot
            scores = dst_weight[columns][:, None, :] + (dual_g[columns][:, None, :] - cost_tile) / EPS
            scores = jnp.where(active_row[:, None, None], scores, NEGATIVE)
            row_top = jnp.max(scores, axis=(0, 2))
            row_sum = jnp.sum(jnp.exp(scores - row_top[None, :, None]), axis=(0, 2))
            block_f = -EPS * (row_top + jnp.log(row_sum))
            col_scores = row_weight[None, :, None] + (block_f[None, :, None] - cost_tile) / EPS
            tile_top = jnp.max(col_scores, axis=1)
            tile_sum = jnp.sum(jnp.exp(col_scores - tile_top[:, None, :]), axis=1)
            tile_top = jnp.where(active_row[:, None], tile_top, NEGATIVE)
            tile_sum = jnp.where(active_row[:, None], tile_sum, 0.0)
            new_top = col_top.at[columns].max(tile_top)
            added = jnp.zeros_like(col_sum).at[columns].add(tile_sum * jnp.exp(tile_top - new_top[columns]))
            new_sum = col_sum * jnp.exp(col_top - new_top) + added
            return (new_top, new_sum), block_f

        initial = (jnp.full((blocks, BLOCK), NEGATIVE, dtype=jnp.float32), jnp.zeros((blocks, BLOCK), dtype=jnp.float32))
        (col_top, col_sum), dual_f = lax.scan(one_block, initial, (src_full, src_half, src_weight, pair_lists, active))
        dual_g = -EPS * (col_top + jnp.log(col_sum))
    return dual_f.reshape(-1), dual_g.reshape(-1)
```

```python
import functools
import math

import jax
import jax.numpy as jnp
from jax import lax
from jax.experimental import pallas as pl
from jax.experimental.pallas import tpu as pltpu
from jax.sharding import PartitionSpec as P

REACH = 3
SPOTS = 2 * REACH + 1
EPS = 0.25
NEGATIVE = -1e30
LOG2E = math.log2(math.e)
SCALE = LOG2E / EPS
BACK = EPS / LOG2E
TAIL = 16
LANES = 128
CHUNK = 16

f32 = jnp.float32
bf16 = jnp.bfloat16


def pieces(value):
    high = value.astype(bf16).astype(f32)
    rest = value - high
    middle = rest.astype(bf16).astype(f32)
    low = (rest - middle).astype(bf16).astype(f32)
    return [high, middle, low]


def stacked(rows, width):
    index = lax.broadcasted_iota(jnp.int32, (TAIL, width), 0)
    out = jnp.zeros((TAIL, width), f32)
    for at, row in enumerate(rows):
        out = jnp.where(index == at, row, out)
    return out.astype(bf16)


def half_norms(points):
    wide = points.astype(f32)
    square = wide * wide
    high = square.astype(bf16)
    low = (square - high.astype(f32)).astype(bf16)
    ones = jnp.ones((8, points.shape[1]), bf16)
    dims = (((1,), (1,)), ((), ()))
    total = lax.dot_general(ones, high, dims, preferred_element_type=f32) + lax.dot_general(
        ones, low, dims, preferred_element_type=f32
    )
    return 0.5 * total[0:1]


def log_sum(top, values):
    return top + jnp.log(values) * LOG2E


def merged(parts):
    top = functools.reduce(jnp.maximum, parts)
    return log_sum(top, sum(jnp.exp2(part - top) for part in parts))


def prepare(base, lists, counts, src, dst, src_lw, dst_lw, start, src_pay, dst_pay, halves):
    block = src.shape[0]
    width = src.shape[1]
    src_half = half_norms(src[...])
    dst_half = half_norms(dst[...])
    halves[0:1, :] = src_half
    halves[1:2, :] = dst_half
    lane = lax.broadcasted_iota(jnp.int32, (1, width), 1) + base[0]
    count = counts[0]
    paired = jnp.zeros((1, width), f32)
    for entry in range(lists.shape[1]):
        column = jnp.where(entry < count, lists[0, entry], lists[0, 0])
        paired = jnp.where(lane == column, 1.0, paired)
    src_pay[0:block, :] = src[...]
    src_pay[block:, :] = stacked(pieces(src_lw[...] * LOG2E) + [paired], width)
    dst_pay[0:block, :] = dst[...]
    weight = dst_lw[...] * LOG2E
    first = weight + (start[...] - dst_half) * SCALE
    dst_pay[block:, :] = stacked(pieces(first) + pieces(weight), width)


def sweep(rows_ref, cols_ref, value_of, bias_ref, dots, tops, sums, bias_row, emit):
    row_blocks = rows_ref.shape[0]
    col_blocks = cols_ref.shape[0]
    block = tops.shape[0]

    def one(at, carry):
        for k in range(col_blocks):
            dots[:, k * block : (k + 1) * block] = lax.dot_general(
                rows_ref[at, 0:block, :],
                cols_ref[k, 0:block, :],
                (((1,), (1,)), ((), ())),
                preferred_element_type=f32,
            )
            bias_row[:, k * block : (k + 1) * block] = (
                value_of(k) + bias_ref[pl.ds(at, 1), k * block : (k + 1) * block]
            )

        def chunk(step, inner):
            start = pl.multiple_of(step * CHUNK, CHUNK)
            parts = [
                dots[pl.ds(start, CHUNK), lane : lane + LANES] * SCALE
                + bias_row[:, lane : lane + LANES]
                for lane in range(0, col_blocks * block, LANES)
            ]
            top = functools.reduce(jnp.maximum, parts)
            tops[pl.ds(start, CHUNK), :] = top
            sums[pl.ds(start, CHUNK), :] = sum(jnp.exp2(part - top) for part in parts)
            return inner

        lax.fori_loop(0, block // CHUNK, chunk, 0)
        turned = tops[...].T
        peak = jnp.max(turned, axis=0, keepdims=True)
        total = jnp.sum(sums[...].T * jnp.exp2(turned - peak), axis=0, keepdims=True)
        emit(at, log_sum(peak, total))
        return carry

    lax.fori_loop(0, row_blocks, one, 0)


def first_rows(here, src_pay, dst_pay, out, row_bias, col_bias, src_value, dst_value, dots, tops, sums, line, value):
    helpers = src_pay.shape[0]
    block = tops.shape[0]
    lane = lax.broadcasted_iota(jnp.int32, (1, src_pay.shape[2]), 1)
    for spot in range(SPOTS):
        tail = dst_pay[spot, block:, :].astype(f32)
        value[spot : spot + 1, :] = tail[0:1] + tail[1:2] + tail[2:3]
        dst_value[spot : spot + 1, :] = tail[3:4] + tail[4:5] + tail[5:6]
    for member in range(helpers):
        tail = src_pay[member, block:, :].astype(f32)
        src_value[member : member + 1, :] = tail[0:1] + tail[1:2] + tail[2:3]
        for spot in range(SPOTS):
            own = jnp.where(lane == spot * helpers + here[0], tail[3:4], 0.0)
            bias = jnp.where(jnp.max(own, axis=1, keepdims=True) > 0.5, 0.0, NEGATIVE)
            bias = jnp.broadcast_to(bias, (1, block))
            row_bias[member : member + 1, spot * block : (spot + 1) * block] = bias
            col_bias[spot : spot + 1, member * block : (member + 1) * block] = bias

    def emit(at, row):
        out[pl.ds(at, 1), :] = row

    sweep(src_pay, dst_pay, lambda k: value[k : k + 1, :], row_bias, dots, tops, sums, line, emit)


def later_rows(gathered, dst_value, row_bias, src_pay, dst_pay, out, dots, tops, sums, line, value):
    summed = merged([gathered[k] for k in range(gathered.shape[0])])
    value[...] = jnp.where(summed > 0.5 * NEGATIVE, dst_value[...] - summed, 0.0)

    def emit(at, row):
        out[pl.ds(at, 1), :] = row

    sweep(src_pay, dst_pay, lambda k: value[k : k + 1, :], row_bias, dots, tops, sums, line, emit)


def columns(last, here, gathered, src_value, col_bias, src_pay, dst_pay, *rest):
    if last:
        halves, out, own_f, padded, dots, tops, sums, line, value = rest
    else:
        out, padded, dots, tops, sums, line, value = rest
    rows = merged([gathered[k] for k in range(gathered.shape[0])])
    value[...] = src_value[...] - rows
    if last:
        mine = lax.broadcasted_iota(jnp.int32, rows.shape, 0) == here[1]
        own = jnp.sum(jnp.where(mine, rows, 0.0), axis=0, keepdims=True)
        own_f[...] = halves[0:1, :] - BACK * own
    total = out.shape[0]
    padded[...] = jnp.full(padded.shape, NEGATIVE, f32)

    def emit(at, row):
        padded[pl.ds(at + total + REACH, 1), :] = row

    sweep(dst_pay, src_pay, lambda k: value[k : k + 1, :], col_bias, dots, tops, sums, line, emit)

    def lay(member, carry):
        if last:
            out[pl.ds(member, 1), :] = padded[pl.ds(member - here[0] + total + SPOTS - 1, 1), :]
        else:
            for spot in range(SPOTS):
                out[member, spot : spot + 1, :] = padded[
                    pl.ds(member - here[0] + spot + total + REACH, 1), :
                ]
        return carry

    lax.fori_loop(0, total, lay, 0)


def finish(gathered, halves, own_g):
    total = gathered.shape[0]
    whole = gathered[...]
    top = jnp.max(whole, axis=0, keepdims=True)
    summed = jnp.sum(jnp.exp2(whole - top), axis=0, keepdims=True)
    own_g[...] = halves[1:2, :] - BACK * log_sum(top, summed)


SMEM = pl.BlockSpec(memory_space=pltpu.SMEM)
VMEM = pl.BlockSpec(memory_space=pltpu.VMEM)


def shifted(block, distance):
    devices = range(lax.axis_size("pts"))
    route = [(i - distance, i) for i in devices if i - distance in devices]
    return lax.ppermute(block, "pts", route)


def spread(block):
    nearby = {0: block}
    for heading in (1, -1):
        filled = 1
        while filled < REACH + 1:
            amount = min(filled, REACH + 1 - filled)
            sent = jnp.stack([nearby[-heading * member] for member in range(amount)])
            arrived = shifted(sent, heading * filled)
            for member in range(amount):
                nearby[-heading * (member + filled)] = arrived[member]
            filled += amount
    return jnp.stack([nearby[offset] for offset in range(-REACH, REACH + 1)])


def on_device(src_points, dst_points, src_logw, dst_logw, init_g, pair_lists, pair_counts):
    helpers = lax.axis_size("help")
    total = lax.axis_size("pts")
    pts_here = lax.axis_index("pts").astype(jnp.int32)
    helper_here = lax.axis_index("help").astype(jnp.int32)
    block, width = src_points.shape
    shape = jax.ShapeDtypeStruct
    pay = shape((block + TAIL, width), bf16)
    src_pay, dst_pay, halves = pl.pallas_call(
        prepare,
        out_shape=(pay, pay, shape((2, block), f32)),
        in_specs=[SMEM, SMEM, SMEM] + [VMEM] * 5,
        out_specs=(VMEM,) * 3,
    )(
        ((pts_here - REACH) * helpers)[None],
        pair_lists,
        pair_counts,
        src_points,
        dst_points,
        src_logw[None],
        dst_logw[None],
        init_g[None],
    )
    dst_near = spread(dst_pay)
    src_near = lax.all_gather(src_pay, "help")

    def scratch(row_blocks, col_blocks):
        return [
            pltpu.VMEM((block, col_blocks * block), f32),
            pltpu.VMEM((block, LANES), f32),
            pltpu.VMEM((block, LANES), f32),
            pltpu.VMEM((1, col_blocks * block), f32),
            pltpu.VMEM((col_blocks, block), f32),
        ]

    where_here = jnp.stack([pts_here, helper_here])
    rows_shape = shape((helpers, block), f32)
    row_part, row_bias, col_bias, src_value, dst_value = pl.pallas_call(
        first_rows,
        out_shape=(
            rows_shape,
            shape((helpers, SPOTS * block), f32),
            shape((SPOTS, helpers * block), f32),
            rows_shape,
            shape((SPOTS, block), f32),
        ),
        in_specs=[SMEM, VMEM, VMEM],
        out_specs=(VMEM,) * 5,
        scratch_shapes=scratch(helpers, SPOTS),
    )(helper_here[None], src_near, dst_near)
    padded = pltpu.VMEM((2 * total + 2 * SPOTS, block), f32)
    gathered = lax.all_gather(row_part, "help")
    col_part = pl.pallas_call(
        functools.partial(columns, False),
        out_shape=shape((total, SPOTS, block), f32),
        in_specs=[SMEM] + [VMEM] * 5,
        out_specs=VMEM,
        scratch_shapes=[padded] + scratch(SPOTS, helpers),
    )(where_here, gathered, src_value, col_bias, src_near, dst_near)
    col_all = lax.all_to_all(col_part, "pts", 0, 0)
    row_part = pl.pallas_call(
        later_rows,
        out_shape=rows_shape,
        in_specs=[VMEM] * 5,
        out_specs=VMEM,
        scratch_shapes=scratch(helpers, SPOTS),
    )(col_all, dst_value, row_bias, src_near, dst_near)
    gathered = lax.all_gather(row_part, "help")
    col_part, own_f = pl.pallas_call(
        functools.partial(columns, True),
        out_shape=(shape((total, block), f32), shape((1, block), f32)),
        in_specs=[SMEM] + [VMEM] * 6,
        out_specs=(VMEM, VMEM),
        scratch_shapes=[padded] + scratch(SPOTS, helpers),
    )(where_here, gathered, src_value, col_bias, src_near, dst_near, halves)
    col_all = lax.all_to_all(col_part, "pts", 0, 0)
    own_g = pl.pallas_call(
        finish,
        out_shape=shape((1, block), f32),
        in_specs=[VMEM, VMEM],
        out_specs=VMEM,
    )(col_all, halves)
    return (own_f[0], own_g[0])


def solution(mesh):
    both = ("pts", "help")
    placed = (P(both, None), P(both, None), P(both), P(both), P(both), P(both, None), P(both))
    return jax.shard_map(
        on_device,
        mesh=mesh,
        in_specs=placed,
        out_specs=(P(both), P(both)),
        check_vma=False,
    )
```

```python
import functools
import math

import jax
import jax.numpy as jnp
from jax import lax
from jax.experimental import pallas as pl
from jax.experimental.pallas import tpu as pltpu
from jax.sharding import PartitionSpec as P

REACH = 3
SPOTS = 2 * REACH + 1
EPS = 0.25
NEGATIVE = -1e30
LOG2E = math.log2(math.e)
SCALE = LOG2E / EPS
BACK = EPS / LOG2E
TAIL = 16
LANES = 128
SUBLANES = 8
CHUNK = 64

f32 = jnp.float32
bf16 = jnp.bfloat16


def pieces(value):
    high = value.astype(bf16).astype(f32)
    rest = value - high
    middle = rest.astype(bf16).astype(f32)
    low = (rest - middle).astype(bf16).astype(f32)
    return [high, middle, low]


def stacked(rows, width):
    index = lax.broadcasted_iota(jnp.int32, (TAIL, width), 0)
    out = jnp.zeros((TAIL, width), f32)
    for at, row in enumerate(rows):
        out = jnp.where(index == at, row, out)
    return out.astype(bf16)


def half_norms(points):
    wide = points.astype(f32)
    square = wide * wide
    high = square.astype(bf16)
    low = (square - high.astype(f32)).astype(bf16)
    ones = jnp.ones((8, points.shape[1]), bf16)
    dims = (((1,), (1,)), ((), ()))
    total = lax.dot_general(ones, high, dims, preferred_element_type=f32) + lax.dot_general(
        ones, low, dims, preferred_element_type=f32
    )
    return 0.5 * total[0:1]


def log_sum(top, values):
    return top + jnp.log(values) * LOG2E


def merged(parts):
    top = functools.reduce(jnp.maximum, parts)
    return log_sum(top, sum(jnp.exp2(part - top) for part in parts))


def swap_route(size, step):
    if size & (size - 1) == 0:
        return [(i, i ^ step) for i in range(size)]
    return [((i + step) % size, i) for i in range(size)]


def swap_slot(size, slot, step):
    return slot ^ step if size & (size - 1) == 0 else (slot - step) % size


def exchanges(total):
    if total & (total - 1) == 0:
        steps = [k for k in range(1, total) if any(abs(i - (i ^ k)) <= REACH for i in range(total))]
        if len(steps) <= 2 * REACH:
            return [("xor", step, 0) for step in steps]
    return [("pair", far, turn) for far in range(1, REACH + 1) for turn in range(2)]


def partner(exchange, index):
    kind, step, turn = exchange
    if kind == "xor":
        return index ^ step
    ahead = (index // step) % 2 == turn
    if isinstance(index, int):
        return index + step if ahead else index - step
    return jnp.where(ahead, index + step, index - step)


def prepare(here, lists, counts, src, dst, src_lw, dst_lw, start, src_pay, dst_pay, halves):
    block, width = src.shape
    dst_half = half_norms(dst[...])
    weight = dst_lw[...] * LOG2E
    first = weight + (start[...] - dst_half) * SCALE
    dst_pay[0:block, :] = dst[...]
    dst_pay[block:, :] = stacked(pieces(first) + pieces(weight), width)
    lane = lax.broadcasted_iota(jnp.int32, (1, width), 1) + (here[0] - REACH) * here[2]
    count = counts[0]
    paired = jnp.zeros((1, width), f32)
    for entry in range(lists.shape[1]):
        column = jnp.where(entry < count, lists[0, entry], lists[0, 0])
        paired = jnp.where(lane == column, 1.0, paired)
    src_pay[0:block, :] = src[...]
    src_pay[block:, :] = stacked(pieces(src_lw[...] * LOG2E) + [paired], width)
    halves[0:1, :] = half_norms(src[...])
    halves[1:2, :] = dst_half


def product(left, right, block):
    return lax.dot_general(
        left[0:block, :], right[0:block, :], (((1,), (1,)), ((), ())), preferred_element_type=f32
    )


def row_sums(src, dst, values, bias, out, dots, tops, sums):
    block = tops.shape[1]

    def multiply(at):
        for k, cols in enumerate(dst):
            dots[at % 2, :, k * block : (k + 1) * block] = product(src[at], cols, block)

    multiply(0)
    for at in range(len(src)):
        if at + 1 < len(src):
            multiply(at + 1)
        slot = at % 2
        lines = []
        for k, value in enumerate(values):
            line = value + bias[at : at + 1, k * block : (k + 1) * block]
            lines += [
                jnp.broadcast_to(line[:, lane : lane + LANES], (SUBLANES, LANES))
                for lane in range(0, block, LANES)
            ]
        for row in range(0, block, SUBLANES):
            parts = [
                dots[slot, row : row + SUBLANES, k * LANES : (k + 1) * LANES] * SCALE + line
                for k, line in enumerate(lines)
            ]
            top = functools.reduce(jnp.maximum, parts)
            tops[slot, row : row + SUBLANES, :] = top
            sums[slot, row : row + SUBLANES, :] = sum(jnp.exp2(part - top) for part in parts)
        turned = tops[slot].T
        peak = jnp.max(turned, axis=0, keepdims=True)
        total = jnp.sum(sums[slot].T * jnp.exp2(turned - peak), axis=0, keepdims=True)
        out[at : at + 1, :] = log_sum(peak, total)


def column_sums(src, dst, values, bias, dots, spread, emit):
    block = values[0].shape[1]
    for k, value in enumerate(values):
        spread[k * block : (k + 1) * block, :] = jnp.broadcast_to(value, (LANES, block)).T

    def multiply(at):
        for k, rows in enumerate(src):
            dots[at % 2, k * block : (k + 1) * block, :] = product(rows, dst[at], block)

    multiply(0)
    for at in range(len(dst)):
        if at + 1 < len(dst):
            multiply(at + 1)
        slot = at % 2
        halves = []
        for lane in range(0, block, LANES):
            found = []
            for k in range(len(src)):
                top = summed = None
                for first in range(k * block, (k + 1) * block, CHUNK):
                    parts = [
                        dots[slot, row : row + SUBLANES, lane : lane + LANES] * SCALE
                        + spread[row : row + SUBLANES, :]
                        for row in range(first, first + CHUNK, SUBLANES)
                    ]
                    peak = functools.reduce(jnp.maximum, parts)
                    if top is None:
                        top = peak
                        summed = sum(jnp.exp2(part - top) for part in parts)
                    else:
                        higher = jnp.maximum(top, peak)
                        summed = summed * jnp.exp2(top - higher) + sum(
                            jnp.exp2(part - higher) for part in parts
                        )
                        top = higher
                at_lane = k * block + lane
                found.append((top + bias[at : at + 1, at_lane : at_lane + LANES], summed))
            peak = functools.reduce(jnp.maximum, [top for top, _ in found])
            summed = sum(part * jnp.exp2(top - peak) for top, part in found)
            highest = jnp.max(peak, axis=0, keepdims=True)
            total = jnp.sum(summed * jnp.exp2(peak - highest), axis=0, keepdims=True)
            halves.append(log_sum(highest, total))
        emit(at, jnp.concatenate(halves, axis=1))


def first_rows(routes, here, *refs):
    helpers = here_helpers(refs, routes)
    spots = len(routes) + 1
    src, refs = refs[:helpers], refs[helpers:]
    dst, refs = refs[:spots], refs[spots:]
    out, row_bias, col_bias, src_value, dst_value, dots, tops, sums = refs
    block = tops.shape[1]
    lane = lax.broadcasted_iota(jnp.int32, (1, src[0].shape[1]), 1)
    values = []
    for spot in range(spots):
        tail = dst[spot][block:, :].astype(f32)
        values.append(tail[0:1] + tail[1:2] + tail[2:3])
        dst_value[spot : spot + 1, :] = tail[3:4] + tail[4:5] + tail[5:6]
    groups = [here[0]] + [partner(route, here[0]) for route in routes]
    for member in range(helpers):
        tail = src[member][block:, :].astype(f32)
        src_value[member : member + 1, :] = tail[0:1] + tail[1:2] + tail[2:3]
        for spot, group in enumerate(groups):
            wanted = (group - here[0] + REACH) * here[2] + here[1]
            own = jnp.where(lane == wanted, tail[3:4], 0.0)
            own = jnp.where(jnp.max(own, axis=1, keepdims=True) > 0.5, 0.0, NEGATIVE)
            own = jnp.broadcast_to(own, (1, block))
            row_bias[member : member + 1, spot * block : (spot + 1) * block] = own
            col_bias[spot : spot + 1, member * block : (member + 1) * block] = own
    row_sums(src, dst, values, row_bias, out, dots, tops, sums)


def here_helpers(refs, routes):
    return len(refs) - (len(routes) + 1) - 8


def later_rows(helpers, gathered, dst_value, row_bias, *refs):
    src, refs = refs[:helpers], refs[helpers:]
    dst, (out, dots, tops, sums) = refs[:-4], refs[-4:]
    summed = merged([gathered[k] for k in range(gathered.shape[0])])
    value = jnp.where(summed > 0.5 * NEGATIVE, dst_value[...] - summed, 0.0)
    values = [value[k : k + 1, :] for k in range(len(dst))]
    row_sums(src, dst, values, row_bias, out, dots, tops, sums)


def columns(last, routes, helpers, here, src_value, col_bias, *refs):
    spots = len(routes) + 1
    given, refs = refs[:helpers], refs[helpers:]
    src, refs = refs[:helpers], refs[helpers:]
    dst, refs = refs[:spots], refs[spots:]
    if last:
        halves, out, own_f, padded, dots, spread = refs
    else:
        out, padded, dots, spread = refs
    values = []
    for member in range(helpers):
        summed = merged(
            [
                given[step][(place := swap_slot(helpers, member, step)) : place + 1, :]
                for step in range(helpers)
            ]
        )
        values.append(src_value[member : member + 1, :] - summed)
        if last and member == 0:
            own_f[...] = halves[0:1, :] - BACK * summed
    total = out.shape[0]
    middle = total + SPOTS
    padded[...] = jnp.full(padded.shape, NEGATIVE, f32)
    groups = [here[0]] + [partner(route, here[0]) for route in routes]

    def emit(at, row):
        padded[pl.ds(groups[at] - here[0] + middle, 1), :] = row

    column_sums(src, dst, values, col_bias, dots, spread, emit)

    def lay(member, carry):
        if last:
            out[member] = padded[pl.ds(member - here[0] + middle, 1), :]
        else:
            wanted = [member] + [partner(route, member) for route in routes]
            for spot, group in enumerate(wanted):
                out[member, spot : spot + 1, :] = padded[pl.ds(group - here[0] + middle, 1), :]
        return carry

    lax.fori_loop(0, total, lay, 0)


def finish(gathered, halves, own_g):
    summed = merged([gathered[k] for k in range(gathered.shape[0])])
    own_g[...] = halves[1:2, :] - BACK * summed


SMEM = pl.BlockSpec(memory_space=pltpu.SMEM)
VMEM = pl.BlockSpec(memory_space=pltpu.VMEM)
PARAMS = pltpu.CompilerParams(vmem_limit_bytes=20 * 1024 * 1024)


def kernel(body, out_shape, ins, scratch=()):
    several = isinstance(out_shape, tuple)
    return pl.pallas_call(
        body,
        out_shape=out_shape,
        in_specs=ins,
        out_specs=(VMEM,) * len(out_shape) if several else VMEM,
        scratch_shapes=list(scratch),
        compiler_params=PARAMS,
    )


def on_device(src_points, dst_points, src_logw, dst_logw, init_g, pair_lists, pair_counts):
    helpers = lax.axis_size("help")
    total = lax.axis_size("pts")
    here = jnp.stack(
        [
            lax.axis_index("pts").astype(jnp.int32),
            lax.axis_index("help").astype(jnp.int32),
            jnp.int32(helpers),
        ]
    )
    block, width = src_points.shape
    routes = exchanges(total)
    spots = len(routes) + 1
    shape = jax.ShapeDtypeStruct
    pay = shape((block + TAIL, width), bf16)
    src_pay, dst_pay, halves = kernel(
        prepare, (pay, pay, shape((2, block), f32)), [SMEM] * 3 + [VMEM] * 5
    )(
        here,
        pair_lists,
        pair_counts,
        src_points,
        dst_points,
        src_logw[None],
        dst_logw[None],
        init_g[None],
    )
    dst = [dst_pay]
    for route in routes:
        ends = [(i, partner(route, i)) for i in range(total)]
        ends = [(i, j) for i, j in ends if 0 <= j < total]
        dst.append(lax.ppermute(dst_pay, "pts", ends))

    def traded(value):
        return [value] + [
            lax.ppermute(value, "help", swap_route(helpers, step)) for step in range(1, helpers)
        ]

    src = traded(src_pay)
    row_scratch = [
        pltpu.VMEM((2, block, spots * block), f32),
        pltpu.VMEM((2, block, LANES), f32),
        pltpu.VMEM((2, block, LANES), f32),
    ]
    col_scratch = [
        pltpu.VMEM((2 * total + 2 * SPOTS, block), f32),
        pltpu.VMEM((2, helpers * block, block), f32),
        pltpu.VMEM((helpers * block, LANES), f32),
    ]
    rows_shape = shape((helpers, block), f32)
    row_part, row_bias, col_bias, src_value, dst_value = kernel(
        functools.partial(first_rows, routes),
        (
            rows_shape,
            shape((helpers, spots * block), f32),
            shape((spots, helpers * block), f32),
            rows_shape,
            shape((spots, block), f32),
        ),
        [SMEM] + [VMEM] * (helpers + spots),
        row_scratch,
    )(here, *src, *dst)
    col_part = kernel(
        functools.partial(columns, False, routes, helpers),
        shape((total, spots, block), f32),
        [SMEM] + [VMEM] * (2 + 2 * helpers + spots),
        col_scratch,
    )(here, src_value, col_bias, *traded(row_part), *src, *dst)
    col_all = lax.all_to_all(col_part, "pts", 0, 0)
    row_part = kernel(
        functools.partial(later_rows, helpers),
        rows_shape,
        [VMEM] * (3 + helpers + spots),
        row_scratch,
    )(col_all, dst_value, row_bias, *src, *dst)
    col_part, own_f = kernel(
        functools.partial(columns, True, routes, helpers),
        (shape((total, 1, block), f32), shape((1, block), f32)),
        [SMEM] + [VMEM] * (3 + 2 * helpers + spots),
        col_scratch,
    )(here, src_value, col_bias, *traded(row_part), *src, *dst, halves)
    col_all = lax.all_to_all(col_part, "pts", 0, 0)
    own_g = kernel(finish, shape((1, block), f32), [VMEM, VMEM])(col_all, halves)
    return (own_f[0], own_g[0])


def solution(mesh):
    both = ("pts", "help")
    placed = (P(both, None), P(both, None), P(both), P(both), P(both), P(both, None), P(both))
    return jax.shard_map(
        on_device,
        mesh=mesh,
        in_specs=placed,
        out_specs=(P(both), P(both)),
        check_vma=False,
    )
```
